32 devices in a mesh: grp: 4 (over z), seq: 4 (over y, x), mp: 2 (over core).
Axes of the slice: x: 2, y: 2, z: 4, core: 2. Of those that a mesh axis runs over, the one named last changes fastest.
Arguments:
- queries: bfloat16 [4, 1024, 2048], P('grp', 'seq', 'mp'), may hold values from -400 to 400
- neighbours: bfloat16 [4, 16, 256, 1024], P('grp', 'seq'), may hold values from -6 to 6
- w_key: bfloat16 [1024, 2048], P(('grp', 'seq'), 'mp'), may hold values from -0.1875 to 0.1875
- w_value: bfloat16 [1024, 2048], P(('grp', 'seq'), 'mp'), may hold values from -0.1875 to 0.1875
- lambdas: float32 [16], P('mp'), may hold values from 0.2 to 0.9
- gain: float32 [2048], P('mp'), may hold values from 0.5 to 1.5
- counts: int32 [4], P('grp'), may hold values from 2 to 16, as said below
- d_out: bfloat16 [4, 1024, 2048], P('grp', 'seq', 'mp'), may hold values from -6 to 6
Outputs:
- attended: bfloat16 [4, 1024, 2048], P('grp', 'seq', 'mp')
- d_neigh: float32 [4, 16, 256, 1024], P('grp', 'seq', None, 'mp')
The draws below stay inside these ranges and needn't reach their ends.
Inputs may be any that keep to these rules, and one draw needn't show every extreme that they name: `counts`: at least one sequence has all 16 groups valid.
All inputs are finite; a program needn't handle non-finite values.
Results may differ from the reference program's by a relative error of at most 0.017.
Values may be sent and summed in bfloat16 or wider, within the bound.
A program may use at most 128 MiB of HBM per device.

```python
import jax
import jax.numpy as jnp
from jax import lax

D_ENC = 1024
PAIRS = 16
KDIM = 64
VDIM = 128
GROUP = 64
NEIGH = 2
NLEN = 128
SEQS = 4
GROUPS = 16
TOKENS = 1024


def draw_queries(key, part):
    extent = (SEQS, TOKENS, PAIRS * 2 * KDIM)
    key_base = jax.random.fold_in(key, 11)
    sample = jax.random.truncated_normal(key_base, -6.0, 6.0, extent, jnp.float32)
    return sample.astype(jnp.bfloat16)


def draw_counts(key, part):
    key_base = jax.random.fold_in(key, 21)
    key_full = jax.random.fold_in(key, 22)
    ragged = jax.random.randint(key_base, (SEQS,), 2, GROUPS + 1, jnp.int32)
    full_seq = jax.random.randint(key_full, (), 0, SEQS, jnp.int32)
    which = jnp.arange(SEQS, dtype=jnp.int32)
    return jnp.where(which == full_seq, jnp.int32(GROUPS), ragged).astype(jnp.int32)


def steps_of(own_key, shape, cuts, least, high):
    factor_of, own = 1.0, jax.random.fold_in(own_key, 6)
    for dim, blocks in cuts:
        heights = jnp.exp(jax.random.uniform(jax.random.fold_in(own, dim), (blocks,), jnp.float32, least / len(cuts), high / len(cuts)))
        factor_of = factor_of * jnp.repeat(heights, shape[dim] // blocks).reshape([-1 if axis == dim else 1 for axis in range(len(shape))])
    return factor_of


def bell_draw(key, dims, spread, limit, shards=(), held_as=jnp.bfloat16):
    factor_of = steps_of(key, dims, shards, -0.22, 0.18) if shards else 1.0
    result = jax.random.normal(key, dims, jnp.float32) * spread * factor_of
    return jnp.minimum(jnp.maximum(result, -limit), limit).astype(held_as)


def setup_inputs(seed: int = 0) -> dict:
    keys = jax.random.split(jax.random.key(seed), 9)
    queries = draw_queries(jax.random.fold_in(keys[8], 71), 0)
    neighbours = bell_draw(keys[1], (SEQS, GROUPS, NEIGH * NLEN, D_ENC), 1.0, 6.0, ((0, 4), (1, 4)))
    w_key = bell_draw(keys[2], (D_ENC, PAIRS * 2 * KDIM), D_ENC ** -0.5, 0.1875, ((0, 16), (1, 2)))
    w_value = bell_draw(keys[3], (D_ENC, PAIRS * VDIM), D_ENC ** -0.5, 0.1875, ((0, 16), (1, 2)))
    lambdas = jnp.clip(0.2 + 0.7 * jax.random.uniform(keys[4], (PAIRS,), jnp.float32) ** steps_of(keys[4], (PAIRS,), ((0, 2),), -0.2, 0.2), 0.2, 0.9)
    gain = jnp.clip(1.0 + 0.1 * jax.random.normal(keys[5], (PAIRS * VDIM,), jnp.float32), 0.5, 1.5)
    counts = draw_counts(jax.random.fold_in(keys[8], 71), 0)
    d_out = bell_draw(keys[7], (SEQS, TOKENS, PAIRS * VDIM), 1.0, 6.0, ((0, 4), (1, 4), (2, 2)))
    return dict(queries=queries, neighbours=neighbours, w_key=w_key, w_value=w_value, lambdas=lambdas, gain=gain, counts=counts, d_out=d_out)


epsilon = 1e-06

def reference(queries, neighbours, w_key, w_value, lambdas, gain, counts, d_out):
    row_count = NEIGH * NLEN
    rows_all = GROUPS * row_count
    score_scale = KDIM ** (-0.5)
    gain_heads = gain.reshape(PAIRS, VDIM)
    lambda_b = lambdas[None, :, None, None]

    def one_sequence(items):
        encoded, query_rows, grad_rows, valid_count = items
        flat_enc = encoded.reshape(rows_all, D_ENC)
        key_own = jnp.dot(flat_enc, w_key, preferred_element_type=jnp.float32)
        value_own = jnp.dot(flat_enc, w_value, preferred_element_type=jnp.float32).astype(jnp.bfloat16)
        key_own = key_own.reshape(GROUPS, row_count, PAIRS, 2, KDIM)
        value_own = value_own.reshape(GROUPS, row_count, PAIRS, VDIM)
        key_heads = jnp.concatenate([jnp.zeros_like(key_own[:1]), key_own[:-1]], axis=0).astype(jnp.float32)
        value_heads = jnp.concatenate([jnp.zeros_like(value_own[:1]), value_own[:-1]], axis=0).astype(jnp.float32)
        query_heads = query_rows.reshape(GROUPS, GROUP, PAIRS, 2, KDIM).astype(jnp.float32)
        position = jnp.arange(GROUPS, dtype=jnp.int32)
        active = ((position >= 1) & (position < valid_count)).astype(jnp.float32)[:, None, None, None]
        scores = jnp.einsum('cqhmd,crhmd->chmqr', query_heads, key_heads, precision=lax.Precision.HIGHEST) * score_scale
        soft_maps = jax.nn.softmax(scores, axis=-1)
        mixed_w = (soft_maps[:, :, 0] - lambda_b * soft_maps[:, :, 1]).astype(jnp.bfloat16)
        heads = jnp.einsum('chqr,crhv->cqhv', mixed_w.astype(jnp.float32), value_heads)
        inverse = lax.rsqrt(lax.optimization_barrier(jnp.mean(heads * heads, axis=-1, keepdims=True)) + epsilon)
        normed = heads * inverse
        attended = (normed * gain_heads * active).astype(jnp.bfloat16).reshape(TOKENS, PAIRS * VDIM)
        upstream = grad_rows.reshape(GROUPS, GROUP, PAIRS, VDIM).astype(jnp.float32) * active
        d_normed = upstream * gain_heads
        d_heads = (inverse * (d_normed - normed * lax.optimization_barrier(jnp.mean(d_normed * normed, axis=-1, keepdims=True)))).astype(jnp.bfloat16)
        d_heads = d_heads.astype(jnp.float32)
        d_mixed = jnp.einsum('cqhv,crhv->chqr', d_heads, value_heads)
        d_values = jnp.einsum('chqr,cqhv->crhv', mixed_w.astype(jnp.float32), d_heads).astype(jnp.bfloat16)
        d_probs = jnp.stack([d_mixed, -lambda_b * d_mixed], axis=2)
        d_scores = (score_scale * soft_maps * (d_probs - lax.optimization_barrier(jnp.sum(d_probs * soft_maps, axis=-1, keepdims=True)))).astype(jnp.bfloat16)
        d_keys = jnp.einsum('chmqr,cqhmd->crhmd', d_scores.astype(jnp.float32), query_heads).astype(jnp.bfloat16)
        d_slots = jnp.dot(d_keys.reshape(rows_all, PAIRS * 2 * KDIM), w_key.T, preferred_element_type=jnp.float32)
        d_slots = d_slots + jnp.dot(d_values.reshape(rows_all, PAIRS * VDIM), w_value.T, preferred_element_type=jnp.float32)
        d_slots = d_slots.reshape(GROUPS, row_count, D_ENC)
        d_enc = jnp.concatenate([d_slots[1:], jnp.zeros_like(d_slots[:1])], axis=0)
        return (attended, d_enc)
    attended, d_neigh = lax.map(one_sequence, (neighbours, queries, d_out, counts))
    return (attended, d_neigh)
```

```python
import functools

import jax
import jax.numpy as jnp
from jax import lax
from jax.experimental import pallas as pl
from jax.experimental.pallas import tpu as pltpu
from jax.sharding import PartitionSpec as P

EPSILON = 1e-06
MESH = pl.DeviceIdType.MESH
NT = (((1,), (1,)), ((), ()))
TN = (((0,), (0,)), ((), ()))


def dot(left, right, dims=(((1,), (0,)), ((), ()))):
    return lax.dot_general(left, right, dims, preferred_element_type=jnp.float32)


def kernel(
    sizes,
    lambdas,
    counts,
    q_hbm,
    n_hbm,
    wk_hbm,
    wv_hbm,
    gain,
    do_hbm,
    att,
    d_out,
    x,
    q,
    do,
    wk,
    wv,
    acc,
    send,
    got,
    edge,
    local_sem,
    own_sem,
    x_send,
    x_recv,
    p1_send,
    p1_recv,
    p2_send,
    p2_recv,
    g_send,
    g_recv,
    e_send,
    e_recv,
):
    n_grp, n_seq, n_mp, w_seq, chunks, pairs = sizes
    groups, rows, enc = x.shape
    group_len = q.shape[0] // groups
    cols = wk.shape[-1]
    pair_cols = cols // pairs
    head_dim = pair_cols // 2
    half = enc // n_mp
    grp, seq, mp = lax.axis_index("grp"), lax.axis_index("seq"), lax.axis_index("mp")
    w_pos = seq if w_seq > 1 else 0
    following = lax.rem(seq + 1, n_seq)
    preceding = lax.rem(seq + n_seq - 1, n_seq)

    own = []
    for c in range(chunks):
        for kind, (src, dst) in enumerate(((wk_hbm, wk), (wv_hbm, wv))):
            own.append(
                pltpu.make_async_copy(
                    src.at[:, pl.ds(c * cols, cols)], dst.at[c, grp, w_pos], own_sem.at[c, kind]
                )
            )
    for copy in own:
        copy.start()
    local = [
        pltpu.make_async_copy(n_hbm.at[pl.ds(0, groups - 1)], x.at[pl.ds(1, groups - 1)], local_sem.at[0]),
        pltpu.make_async_copy(q_hbm, q, local_sem.at[1]),
        pltpu.make_async_copy(do_hbm, do, local_sem.at[2]),
    ]
    for copy in local:
        copy.start()

    others = [{"grp": lax.rem(grp + o, n_grp)} for o in range(1, n_grp)]
    others += [{"seq": lax.rem(seq + o, n_seq)} for o in (range(1, n_seq) if w_seq > 1 else (1, n_seq - 1))]
    for o in range(1, n_mp):
        partner = lax.rem(mp + o, n_mp)
        others += [{"mp": partner}, {"seq": following, "mp": partner}, {"seq": preceding, "mp": partner}]
    barrier = pltpu.get_barrier_semaphore()
    for device in others:
        pl.semaphore_signal(barrier, inc=1, device_id=device, device_id_type=MESH)
    pl.semaphore_wait(barrier, len(others))

    def remote(src, dst, send_sem, recv_sem, device):
        return pltpu.make_async_remote_copy(
            src_ref=src, dst_ref=dst, send_sem=send_sem, recv_sem=recv_sem, device_id=device, device_id_type=MESH
        )

    def over_grp(ref, sems, c, kind, block):
        return [
            remote(block, block, sems[0].at[c, kind, o], sems[1].at[c, kind, o], {"grp": lax.rem(grp + o, n_grp)})
            for o in range(1, n_grp)
        ]

    def over_seq(ref, sems, c, kind, block):
        return [
            remote(block, block, sems[0].at[c, kind, o], sems[1].at[c, kind, o], {"seq": lax.rem(seq + o, n_seq)})
            for o in range(1, w_seq)
        ]

    one, two = (p1_send, p1_recv), (p2_send, p2_recv)
    first = [
        over_seq(wk, one, c, 0, wk.at[c, grp, w_pos]) + over_grp(wv, one, c, 1, wv.at[c, grp, w_pos])
        for c in range(chunks)
    ]
    second = [
        over_grp(wk, two, c, 0, wk.at[c, grp]) + over_seq(wv, two, c, 1, wv.at[c, :, w_pos]) for c in range(chunks)
    ]
    edge_in = remote(n_hbm.at[groups - 1], x.at[0], x_send, x_recv, {"seq": following})

    def start_first(c):
        own[2 * c].wait()
        own[2 * c + 1].wait()
        for copy in first[c]:
            copy.start()

    def start_second(c):
        for copy in first[c]:
            copy.wait_recv()
        for copy in second[c]:
            copy.start()

    start_first(0)
    edge_in.start()
    for c in range(1, chunks):
        start_first(c)
        start_second(c - 1)
    start_second(chunks - 1)

    for copy in local:
        copy.wait()
    edge_in.wait_recv()

    scale = head_dim ** (-0.5)
    lane = lax.broadcasted_iota(jnp.int32, (group_len, pair_cols), 1)
    on_first = lane < head_dim

    def slot_step(c, u):
        w_k = wk[c].reshape(enc, cols)
        w_v = wv[c].reshape(enc, cols)
        enc_rows = x[u]
        keys = dot(enc_rows, w_k)
        vals = dot(enc_rows, w_v).astype(jnp.bfloat16)
        position = seq * groups + u
        active = (jnp.clip(position, 0, 1) * jnp.clip(counts[0] - position, 0, 1)).astype(jnp.float32)
        tokens = pl.ds(pl.multiple_of(u * group_len, group_len), group_len)
        d_keys, d_vals = [], []
        for p in range(pairs):
            at = pl.ds((c * pairs + p) * pair_cols, pair_cols)
            here = slice(p * pair_cols, (p + 1) * pair_cols)
            lam = lambdas[c * pairs + p]
            query = q[tokens, at]
            zero = jnp.zeros_like(query)
            q2 = jnp.concatenate([jnp.where(on_first, query, zero), jnp.where(on_first, zero, query)], axis=0)
            key = keys[:, here]
            value = vals[:, here]
            key_hi = key.astype(jnp.bfloat16)
            key_lo = (key - key_hi.astype(jnp.float32)).astype(jnp.bfloat16)
            scores = (
                dot(jnp.concatenate([q2, q2], axis=1), jnp.concatenate([key_hi, key_lo], axis=1), NT) * scale
            )
            top = jnp.max(scores, axis=-1, keepdims=True)
            e = jnp.exp(scores - top)
            probs = e * (1.0 / jnp.sum(e, axis=-1, keepdims=True))
            mix = (probs[:group_len] - lam * probs[group_len:]).astype(jnp.bfloat16)
            heads = dot(mix, value)
            inverse = lax.rsqrt(jnp.mean(heads * heads, axis=-1, keepdims=True) + EPSILON)
            normed = heads * inverse
            g = gain[:, at]
            att[tokens, at] = (normed * g * active).astype(jnp.bfloat16)
            dn = do[tokens, at].astype(jnp.float32) * active * g
            d_heads = (inverse * (dn - normed * jnp.mean(dn * normed, axis=-1, keepdims=True))).astype(jnp.bfloat16)
            d_mix = dot(d_heads, value, NT)
            d_vals.append(dot(mix, d_heads, TN).astype(jnp.bfloat16))
            d_probs = jnp.concatenate([d_mix, -lam * d_mix], axis=0)
            total = jnp.sum(d_probs * probs, axis=-1, keepdims=True)
            d_scores = (scale * probs * (d_probs - total)).astype(jnp.bfloat16)
            d_keys.append(dot(d_scores, q2, TN).astype(jnp.bfloat16))
        grad = dot(jnp.concatenate(d_keys, axis=1), w_k, NT) + dot(jnp.concatenate(d_vals, axis=1), w_v, NT)
        if c == 0:
            acc[u] = grad
        else:
            acc[u] += grad

    def arrived(c):
        for copy in second[c]:
            copy.wait_recv()

    for c in range(chunks - 1):
        arrived(c)

        def step(u, carry, c=c):
            slot_step(c, u)
            return carry

        lax.fori_loop(0, groups, step, 0)

    last = chunks - 1
    arrived(last)
    mine = pl.ds(pl.multiple_of(mp * half, half), half)

    slot_step(last, 0)
    edge_out = []
    for o in range(n_mp):
        core = lax.rem(mp + o, n_mp)
        send[0, o] = acc[0, :, pl.ds(pl.multiple_of(core * half, half), half)].astype(jnp.bfloat16)
        edge_out.append(
            remote(send.at[0, o], edge.at[o], e_send.at[o], e_recv.at[o], {"seq": preceding, "mp": core})
        )
    for copy in edge_out:
        copy.start()

    def exchange(u, o):
        return remote(
            send.at[u, o], got.at[u, o], g_send.at[u, o], g_recv.at[u, o], {"mp": lax.rem(mp + o, n_mp)}
        )

    def last_step(u, carry):
        slot_step(last, u)
        for o in range(1, n_mp):
            core = lax.rem(mp + o, n_mp)
            send[u, o] = acc[u, :, pl.ds(pl.multiple_of(core * half, half), half)].astype(jnp.bfloat16)
            exchange(u, o).start()
        return carry

    lax.fori_loop(1, groups, last_step, 0)

    for copy in edge_out:
        copy.wait()
    total = edge[0].astype(jnp.float32)
    for o in range(1, n_mp):
        total += edge[o].astype(jnp.float32)
    d_out[groups - 1] = total

    def finish(u, carry):
        total = acc[u, :, mine]
        for o in range(1, n_mp):
            exchange(u, o).wait()
            total += got[u, o].astype(jnp.float32)
        d_out[u - 1] = total
        return carry

    lax.fori_loop(1, groups, finish, 0)
    for c in range(chunks):
        for copy in first[c] + second[c]:
            copy.wait_send()
    edge_in.wait_send()


def on_device(mesh_shape, queries, neighbours, w_key, w_value, lambdas, gain, counts, d_out):
    n_grp, n_seq, n_mp = (mesh_shape[name] for name in ("grp", "seq", "mp"))
    groups, rows, enc = neighbours.shape[1:]
    tokens, width = queries.shape[1:]
    w_seq = n_seq
    if w_key.shape[0] % 16:
        w_key = lax.all_gather(w_key, "seq", axis=0, tiled=True)
        w_value = lax.all_gather(w_value, "seq", axis=0, tiled=True)
        w_seq = 1
    w_rows = w_key.shape[0]
    pair_count = lambdas.shape[0]
    pairs = 2 if pair_count % 2 == 0 else 1
    chunks = pair_count // pairs
    cols = w_key.shape[1] // chunks
    half = enc // n_mp
    bf16, f32 = jnp.bfloat16, jnp.float32
    vmem = pl.BlockSpec(memory_space=pltpu.VMEM)
    smem = pl.BlockSpec(memory_space=pltpu.SMEM)
    hbm = pl.BlockSpec(memory_space=pl.ANY)
    dma = pltpu.SemaphoreType.DMA
    att, d_neigh = pl.pallas_call(
        functools.partial(kernel, (n_grp, n_seq, n_mp, w_seq, chunks, pairs)),
        out_shape=(
            jax.ShapeDtypeStruct((tokens, width), bf16),
            jax.ShapeDtypeStruct((groups, rows, half), f32),
        ),
        in_specs=[smem, smem, hbm, hbm, hbm, hbm, vmem, hbm],
        out_specs=(vmem, vmem),
        scratch_shapes=[
            pltpu.VMEM((groups, rows, enc), bf16),
            pltpu.VMEM((tokens, width), bf16),
            pltpu.VMEM((tokens, width), bf16),
            pltpu.VMEM((chunks, n_grp, w_seq, w_rows, cols), bf16),
            pltpu.VMEM((chunks, n_grp, w_seq, w_rows, cols), bf16),
            pltpu.VMEM((groups, rows, enc), f32),
            pltpu.VMEM((groups, n_mp, rows, half), bf16),
            pltpu.VMEM((groups, n_mp, rows, half), bf16),
            pltpu.VMEM((n_mp, rows, half), bf16),
            dma((3,)),
            dma((chunks, 2)),
            dma,
            dma,
            dma((chunks, 2, max(n_grp, w_seq))),
            dma((chunks, 2, max(n_grp, w_seq))),
            dma((chunks, 2, max(n_grp, w_seq))),
            dma((chunks, 2, max(n_grp, w_seq))),
            dma((groups, n_mp)),
            dma((groups, n_mp)),
            dma((n_mp,)),
            dma((n_mp,)),
        ],
        compiler_params=pltpu.CompilerParams(
            collective_id=0, has_side_effects=True, vmem_limit_bytes=60 * 1024 * 1024
        ),
    )(lambdas, counts, queries[0], neighbours[0], w_key, w_value, gain.reshape(1, -1), d_out[0])
    return att[None], d_neigh[None]


def solution(mesh):
    in_specs = (
        P("grp", "seq", "mp"),
        P("grp", "seq", None, None),
        P(("grp", "seq"), "mp"),
        P(("grp", "seq"), "mp"),
        P("mp"),
        P("mp"),
        P("grp"),
        P("grp", "seq", "mp"),
    )
    out_specs = (P("grp", "seq", "mp"), P("grp", "seq", None, "mp"))
    return jax.shard_map(
        functools.partial(on_device, dict(mesh.shape)),
        mesh=mesh,
        in_specs=in_specs,
        out_specs=out_specs,
        check_vma=False,
    )
```

```python
import functools

import jax
import jax.numpy as jnp
from jax import lax
from jax.experimental import pallas as pl
from jax.experimental.pallas import tpu as pltpu
from jax.sharding import PartitionSpec as P

EPSILON = 1e-06
MESH = pl.DeviceIdType.MESH
NT = (((1,), (1,)), ((), ()))
TN = (((0,), (0,)), ((), ()))


def dot(left, right, dims=(((1,), (0,)), ((), ()))):
    return lax.dot_general(left, right, dims, preferred_element_type=jnp.float32)


def kernel(
    sizes,
    lambdas,
    counts,
    q_hbm,
    n_hbm,
    wk_hbm,
    wv_hbm,
    gain,
    do_hbm,
    att,
    d_out,
    x,
    q,
    do,
    wk,
    wv,
    acc,
    send,
    got,
    edge,
    local_sem,
    own_sem,
    x_send,
    x_recv,
    p1_send,
    p1_recv,
    p2_send,
    p2_recv,
    g_send,
    g_recv,
    e_send,
    e_recv,
):
    n_grp, n_seq, n_mp, w_seq, chunks, pairs = sizes
    groups, rows, enc = x.shape
    group_len = q.shape[0] // groups
    cols = wk.shape[-1]
    pair_cols = cols // pairs
    head_dim = pair_cols // 2
    half = enc // n_mp
    grp, seq, mp = lax.axis_index("grp"), lax.axis_index("seq"), lax.axis_index("mp")
    w_pos = seq if w_seq > 1 else 0
    following = lax.rem(seq + 1, n_seq)
    preceding = lax.rem(seq + n_seq - 1, n_seq)

    own = []
    for c in range(chunks):
        for kind, (src, dst) in enumerate(((wk_hbm, wk), (wv_hbm, wv))):
            own.append(
                pltpu.make_async_copy(
                    src.at[:, pl.ds(c * cols, cols)], dst.at[c, grp, w_pos], own_sem.at[c, kind]
                )
            )
    for copy in own:
        copy.start()
    local = [
        pltpu.make_async_copy(n_hbm.at[pl.ds(0, groups - 1)], x.at[pl.ds(1, groups - 1)], local_sem.at[0]),
        pltpu.make_async_copy(q_hbm, q, local_sem.at[1]),
        pltpu.make_async_copy(do_hbm, do, local_sem.at[2]),
    ]
    for copy in local:
        copy.start()

    others = [{"grp": lax.rem(grp + o, n_grp)} for o in range(1, n_grp)]
    others += [{"seq": lax.rem(seq + o, n_seq)} for o in (range(1, n_seq) if w_seq > 1 else (1, n_seq - 1))]
    for o in range(1, n_mp):
        partner = lax.rem(mp + o, n_mp)
        others += [{"mp": partner}, {"seq": following, "mp": partner}, {"seq": preceding, "mp": partner}]
    barrier = pltpu.get_barrier_semaphore()
    for device in others:
        pl.semaphore_signal(barrier, inc=1, device_id=device, device_id_type=MESH)
    pl.semaphore_wait(barrier, len(others))

    def remote(src, dst, send_sem, recv_sem, device):
        return pltpu.make_async_remote_copy(
            src_ref=src, dst_ref=dst, send_sem=send_sem, recv_sem=recv_sem, device_id=device, device_id_type=MESH
        )

    def over_grp(sems, c, kind, block):
        return [
            remote(block, block, sems[0].at[c, kind, o], sems[1].at[c, kind, o], {"grp": lax.rem(grp + o, n_grp)})
            for o in range(1, n_grp)
        ]

    def over_seq(sems, c, kind, block):
        return [
            remote(block, block, sems[0].at[c, kind, o], sems[1].at[c, kind, o], {"seq": lax.rem(seq + o, n_seq)})
            for o in range(1, w_seq)
        ]

    first, second, onward = [], [], []
    for c in range(chunks):
        early, late, relay = [], [], []
        for kind, ref in enumerate((wk, wv)):
            early += over_grp((p1_send, p1_recv), c, kind, ref.at[c, grp, w_pos])
            block = ref.at[c, :, w_pos]
            if w_seq == 4:
                right = lax.rem(seq, 2) * 2 + 1 - seq // 2
                left = (1 - lax.rem(seq, 2)) * 2 + seq // 2
                for o, device in ((1, right), (2, left)):
                    late.append(
                        remote(block, block, p2_send.at[c, kind, o], p2_recv.at[c, kind, o], {"seq": device})
                    )
                source, target = (left, right) if kind == 0 else (right, left)
                passed = ref.at[c, :, source]
                relay.append(
                    (
                        late[2 * kind + kind],
                        remote(passed, passed, p2_send.at[c, kind, 3], p2_recv.at[c, kind, 3], {"seq": target}),
                    )
                )
            else:
                late += over_seq((p2_send, p2_recv), c, kind, block)
        first.append(early)
        second.append(late)
        onward.append(relay)
    part = pl.ds(pl.multiple_of(mp * (rows // n_mp), rows // n_mp), rows // n_mp)
    edge_in = remote(n_hbm.at[groups - 1, part], x.at[0, part], x_send.at[0], x_recv.at[0], {"seq": following})
    edge_on = [
        remote(x.at[0, part], x.at[0, part], x_send.at[o], x_recv.at[o], {"mp": lax.rem(mp + o, n_mp)})
        for o in range(1, n_mp)
    ]

    def start_first(c):
        if c < chunks:
            own[2 * c].wait()
            own[2 * c + 1].wait()
            for copy in first[c]:
                copy.start()

    def start_second(c):
        if c < chunks:
            for copy in first[c]:
                copy.wait_recv()
            for copy in second[c]:
                copy.start()
            start_first(c + 2)

    def start_onward(c):
        if c < chunks:
            for arrival, copy in onward[c]:
                arrival.wait_recv()
                copy.start()

    def arrived(c):
        passed_on = [arrival for arrival, _ in onward[c]]
        for copy in second[c] + [copy for _, copy in onward[c]]:
            if not any(copy is other for other in passed_on):
                copy.wait_recv()
        start_second(c + 2)
        start_onward(c + 1)

    start_first(0)
    edge_in.start()
    start_first(1)
    start_second(0)
    edge_in.wait_recv()
    for copy in edge_on:
        copy.start()
    start_second(1)
    start_onward(0)
    for copy in local:
        copy.wait()
    for copy in edge_on:
        copy.wait_recv()

    scale = head_dim ** (-0.5)
    lane = lax.broadcasted_iota(jnp.int32, (group_len, pair_cols), 1)
    on_first = lane < head_dim

    def slot_step(c, u):
        w_k = wk[c].reshape(enc, cols)
        w_v = wv[c].reshape(enc, cols)
        enc_rows = x[u]
        keys = dot(enc_rows, w_k)
        vals = dot(enc_rows, w_v).astype(jnp.bfloat16)
        position = seq * groups + u
        active = (jnp.clip(position, 0, 1) * jnp.clip(counts[0] - position, 0, 1)).astype(jnp.float32)
        tokens = pl.ds(pl.multiple_of(u * group_len, group_len), group_len)
        d_keys, d_vals = [], []
        for p in range(pairs):
            at = pl.ds((c * pairs + p) * pair_cols, pair_cols)
            here = slice(p * pair_cols, (p + 1) * pair_cols)
            lam = lambdas[c * pairs + p]
            query = q[tokens, at]
            zero = jnp.zeros_like(query)
            q2 = jnp.concatenate([jnp.where(on_first, query, zero), jnp.where(on_first, zero, query)], axis=0)
            key = keys[:, here]
            value = vals[:, here]
            key_hi = key.astype(jnp.bfloat16)
            key_lo = (key - key_hi.astype(jnp.float32)).astype(jnp.bfloat16)
            scores = (
                dot(jnp.concatenate([q2, q2], axis=1), jnp.concatenate([key_hi, key_lo], axis=1), NT) * scale
            )
            top = jnp.max(scores, axis=-1, keepdims=True)
            e = jnp.exp(scores - top)
            probs = e * (1.0 / jnp.sum(e, axis=-1, keepdims=True))
            mix = (probs[:group_len] - lam * probs[group_len:]).astype(jnp.bfloat16)
            heads = dot(mix, value)
            inverse = lax.rsqrt(jnp.mean(heads * heads, axis=-1, keepdims=True) + EPSILON)
            normed = heads * inverse
            g = gain[:, at]
            att[tokens, at] = (normed * g * active).astype(jnp.bfloat16)
            dn = do[tokens, at].astype(jnp.float32) * active * g
            d_heads = (inverse * (dn - normed * jnp.mean(dn * normed, axis=-1, keepdims=True))).astype(jnp.bfloat16)
            d_mix = dot(d_heads, value, NT)
            d_vals.append(dot(mix, d_heads, TN).astype(jnp.bfloat16))
            d_probs = jnp.concatenate([d_mix, -lam * d_mix], axis=0)
            total = jnp.sum(d_probs * probs, axis=-1, keepdims=True)
            d_scores = (scale * probs * (d_probs - total)).astype(jnp.bfloat16)
            d_keys.append(dot(d_scores, q2, TN).astype(jnp.bfloat16))
        grad = dot(jnp.concatenate(d_keys, axis=1), w_k, NT) + dot(jnp.concatenate(d_vals, axis=1), w_v, NT)
        if c == 0:
            acc[u] = grad
        else:
            acc[u] += grad

    for c in range(chunks - 1):
        arrived(c)

        def step(u, carry, c=c):
            slot_step(c, u)
            return carry

        lax.fori_loop(0, groups, step, 0)

    last = chunks - 1
    arrived(last)
    mine = pl.ds(pl.multiple_of(mp * half, half), half)

    slot_step(last, 0)
    edge_out = []
    for o in range(n_mp):
        core = lax.rem(mp + o, n_mp)
        send[0, o] = acc[0, :, pl.ds(pl.multiple_of(core * half, half), half)].astype(jnp.bfloat16)
        edge_out.append(
            remote(send.at[0, o], edge.at[o], e_send.at[o], e_recv.at[o], {"seq": preceding, "mp": core})
        )
    for copy in edge_out:
        copy.start()

    def exchange(u, o):
        return remote(
            send.at[u, o], got.at[u, o], g_send.at[u, o], g_recv.at[u, o], {"mp": lax.rem(mp + o, n_mp)}
        )

    def last_step(u, carry):
        slot_step(last, u)
        for o in range(1, n_mp):
            core = lax.rem(mp + o, n_mp)
            send[u, o] = acc[u, :, pl.ds(pl.multiple_of(core * half, half), half)].astype(jnp.bfloat16)
            exchange(u, o).start()
        return carry

    lax.fori_loop(1, groups, last_step, 0)

    for copy in edge_out:
        copy.wait()
    total = edge[0].astype(jnp.float32)
    for o in range(1, n_mp):
        total += edge[o].astype(jnp.float32)
    d_out[groups - 1] = total

    def finish(u, carry):
        total = acc[u, :, mine]
        for o in range(1, n_mp):
            exchange(u, o).wait()
            total += got[u, o].astype(jnp.float32)
        d_out[u - 1] = total
        return carry

    lax.fori_loop(1, groups, finish, 0)
    for c in range(chunks):
        for copy in first[c] + second[c] + [copy for _, copy in onward[c]]:
            copy.wait_send()
    edge_in.wait_send()
    for copy in edge_on:
        copy.wait_send()


def on_device(mesh_shape, queries, neighbours, w_key, w_value, lambdas, gain, counts, d_out):
    n_grp, n_seq, n_mp = (mesh_shape[name] for name in ("grp", "seq", "mp"))
    groups, rows, enc = neighbours.shape[1:]
    tokens, width = queries.shape[1:]
    w_seq = n_seq
    if w_key.shape[0] % 16:
        w_key = lax.all_gather(w_key, "seq", axis=0, tiled=True)
        w_value = lax.all_gather(w_value, "seq", axis=0, tiled=True)
        w_seq = 1
    w_rows = w_key.shape[0]
    pair_count = lambdas.shape[0]
    pairs = 2 if pair_count % 2 == 0 else 1
    chunks = pair_count // pairs
    cols = w_key.shape[1] // chunks
    half = enc // n_mp
    bf16, f32 = jnp.bfloat16, jnp.float32
    vmem = pl.BlockSpec(memory_space=pltpu.VMEM)
    smem = pl.BlockSpec(memory_space=pltpu.SMEM)
    hbm = pl.BlockSpec(memory_space=pl.ANY)
    dma = pltpu.SemaphoreType.DMA
    att, d_neigh = pl.pallas_call(
        functools.partial(kernel, (n_grp, n_seq, n_mp, w_seq, chunks, pairs)),
        out_shape=(
            jax.ShapeDtypeStruct((tokens, width), bf16),
            jax.ShapeDtypeStruct((groups, rows, half), f32),
        ),
        in_specs=[smem, smem, hbm, hbm, hbm, hbm, vmem, hbm],
        out_specs=(vmem, vmem),
        scratch_shapes=[
            pltpu.VMEM((groups, rows, enc), bf16),
            pltpu.VMEM((tokens, width), bf16),
            pltpu.VMEM((tokens, width), bf16),
            pltpu.VMEM((chunks, n_grp, w_seq, w_rows, cols), bf16),
            pltpu.VMEM((chunks, n_grp, w_seq, w_rows, cols), bf16),
            pltpu.VMEM((groups, rows, enc), f32),
            pltpu.VMEM((groups, n_mp, rows, half), bf16),
            pltpu.VMEM((groups, n_mp, rows, half), bf16),
            pltpu.VMEM((n_mp, rows, half), bf16),
            dma((3,)),
            dma((chunks, 2)),
            dma((n_mp,)),
            dma((n_mp,)),
            dma((chunks, 2, max(n_grp, w_seq))),
            dma((chunks, 2, max(n_grp, w_seq))),
            dma((chunks, 2, max(n_grp, w_seq))),
            dma((chunks, 2, max(n_grp, w_seq))),
            dma((groups, n_mp)),
            dma((groups, n_mp)),
            dma((n_mp,)),
            dma((n_mp,)),
        ],
        compiler_params=pltpu.CompilerParams(
            collective_id=0, has_side_effects=True, vmem_limit_bytes=60 * 1024 * 1024
        ),
    )(lambdas, counts, queries[0], neighbours[0], w_key, w_value, gain.reshape(1, -1), d_out[0])
    return att[None], d_neigh[None]


def solution(mesh):
    in_specs = (
        P("grp", "seq", "mp"),
        P("grp", "seq", None, None),
        P(("grp", "seq"), "mp"),
        P(("grp", "seq"), "mp"),
        P("mp"),
        P("mp"),
        P("grp"),
        P("grp", "seq", "mp"),
    )
    out_specs = (P("grp", "seq", "mp"), P("grp", "seq", None, "mp"))
    return jax.shard_map(
        functools.partial(on_device, dict(mesh.shape)),
        mesh=mesh,
        in_specs=in_specs,
        out_specs=out_specs,
        check_vma=False,
    )
```
